16 devices in a mesh: dp: 2 (over z), ep: 8 (over y, x, core).
Axes of the slice: x: 2, y: 2, z: 2, core: 2. Of those that a mesh axis runs over, the one named last changes fastest.
Arguments:
- x_tok: bfloat16 [2048, 2048], P(('dp', 'ep')), parts along dimension 0
- topk_idx: int32 [2048, 6], P(('dp', 'ep')), parts along dimension 0
- topk_w: float32 [2048, 6], P(('dp', 'ep')), parts along dimension 0
- w_in: bfloat16 [64, 2048, 1408], P('ep')
- w_out: bfloat16 [64, 1408, 2048], P('ep')
- shared_in: bfloat16 [2048, 2816], replicated
- shared_out: bfloat16 [2816, 2048], replicated
Outputs:
- output: bfloat16 [2048, 2048], P(('dp', 'ep')), parts along dimension 0
There are 2 independent parts. The reference program is written for one: setup_inputs(seed, part) draws one part's arguments, and reference() takes and returns one part's arrays. A program takes and returns all parts, laid end to end along the dimension named above; an argument that names none is the same for every part.
All inputs are finite; a program needn't handle non-finite values.
Results may differ from the reference program's by a relative error of at most 0.001.
Values are sent between devices in bfloat16 or wider.
A program may use at most 1 GiB of HBM per device.

```python
import jax
import jax.numpy as jnp
from jax import lax

GROUP_SIZE = 8
TOK_DEV = 128
D_MODEL = 2048
FF_DIM = 1408
FS_DIM = 2816
EXPERTS = 64
TOP_K = 6
NUM_HOT = 2
SLOT_CAP = 36

TOKENS = GROUP_SIZE * TOK_DEV
EXPERT_ROWS = SLOT_CAP * GROUP_SIZE


def draw_routing(route_key):
    key_hot, key_extra, key_tok, key_rot = jax.random.split(route_key, 4)
    cold_count = EXPERTS - NUM_HOT
    rest_pairs = TOK_DEV * TOP_K - NUM_HOT * SLOT_CAP
    base_load = rest_pairs // cold_count
    extra_pairs = rest_pairs - base_load * cold_count
    expert_order = jax.random.permutation(key_hot, EXPERTS)
    cold_rank = jax.vmap(lambda dev_key: jax.random.permutation(dev_key, cold_count))(jax.random.split(key_extra, GROUP_SIZE))
    cold_load = base_load + (cold_rank < extra_pairs).astype(jnp.int32)
    hot_load = jnp.full((GROUP_SIZE, NUM_HOT), SLOT_CAP, jnp.int32)
    ordered_load = jnp.concatenate([hot_load, cold_load], axis=1)
    expert_load = jnp.zeros((GROUP_SIZE, EXPERTS), jnp.int32).at[:, expert_order].set(ordered_load)
    load_ends = jnp.cumsum(expert_load, axis=1)
    pair_ids = jnp.arange(TOK_DEV * TOP_K, dtype=jnp.int32)
    pair_expert = jax.vmap(lambda ends_row: jnp.searchsorted(ends_row, pair_ids, side='right'))(load_ends)
    slot_table = pair_expert.reshape(GROUP_SIZE, TOP_K, TOK_DEV).transpose(0, 2, 1)
    tok_perm = jax.vmap(lambda dev_key: jax.random.permutation(dev_key, TOK_DEV))(jax.random.split(key_tok, GROUP_SIZE))
    tok_index = jnp.broadcast_to(tok_perm[:, :, None], (GROUP_SIZE, TOK_DEV, TOP_K))
    slot_table = jnp.take_along_axis(slot_table, tok_index, axis=1)
    slot_shift = jax.random.randint(key_rot, (GROUP_SIZE, TOK_DEV, 1), 0, TOP_K)
    slot_cols = (jnp.arange(TOP_K)[None, None, :] + slot_shift) % TOP_K
    slot_table = jnp.take_along_axis(slot_table, slot_cols, axis=2)
    return slot_table.reshape(TOKENS, TOP_K).astype(jnp.int32)


def draw_stack(stack_key, fan_in, fan_out):
    def one_expert(expert_key):
        return (jax.random.normal(expert_key, (fan_in, fan_out), jnp.float32) * fan_in ** -0.5).astype(jnp.bfloat16)
    return lax.map(one_expert, jax.random.split(stack_key, EXPERTS))


def setup_inputs(seed: int = 0, part: int = 0) -> dict:
    root_key = jax.random.key(seed)
    key_x, key_route, key_gate, key_in, key_out, key_sin, key_sout = jax.random.split(root_key, 7)
    x_tok = jax.random.normal(jax.random.fold_in(key_x, part), (TOKENS, D_MODEL), jnp.float32).astype(jnp.bfloat16)
    topk_idx = draw_routing(jax.random.fold_in(key_route, part))
    gate_raw = jax.random.uniform(jax.random.fold_in(key_gate, part), (TOKENS, TOP_K), jnp.float32, 0.2, 1.0)
    topk_w = gate_raw * (1.5 / TOP_K ** 0.5)
    w_in = draw_stack(key_in, D_MODEL, FF_DIM)
    w_out = draw_stack(key_out, FF_DIM, D_MODEL)
    shared_in = (jax.random.normal(key_sin, (D_MODEL, FS_DIM), jnp.float32) * D_MODEL ** -0.5).astype(jnp.bfloat16)
    shared_out = (jax.random.normal(key_sout, (FS_DIM, D_MODEL), jnp.float32) * FS_DIM ** -0.5).astype(jnp.bfloat16)
    return {'x_tok': x_tok, 'topk_idx': topk_idx, 'topk_w': topk_w, 'w_in': w_in, 'w_out': w_out, 'shared_in': shared_in, 'shared_out': shared_out}


def reference(x_tok, topk_idx, topk_w, w_in, w_out, shared_in, shared_out):
    pair_total = TOKENS * TOP_K
    flat_ids = topk_idx.reshape(pair_total)
    pair_order = jnp.argsort(flat_ids, stable=True)
    counts = jnp.zeros((EXPERTS,), jnp.int32).at[flat_ids].add(1)
    starts = jnp.cumsum(counts) - counts
    pair_gates = topk_w.astype(jnp.bfloat16).astype(jnp.float32).reshape(pair_total)
    slot_ids = jnp.arange(EXPERT_ROWS)

    def expert_step(routed_acc, step_in):
        e_index, w_first, w_second = step_in
        slot_valid = slot_ids < counts[e_index]
        pair_pos = pair_order[jnp.minimum(starts[e_index] + slot_ids, pair_total - 1)]
        tok_pos = pair_pos // TOP_K
        gathered = x_tok[tok_pos]
        hidden = jax.nn.gelu(jnp.dot(gathered, w_first, preferred_element_type=jnp.float32), approximate=True).astype(jnp.bfloat16)
        expert_out = jnp.dot(hidden, w_second, preferred_element_type=jnp.float32).astype(jnp.bfloat16)
        pair_scale = jnp.where(slot_valid, pair_gates[pair_pos], 0.0)
        contrib = expert_out.astype(jnp.float32) * pair_scale[:, None]
        return routed_acc.at[tok_pos].add(contrib), None

    routed_init = jnp.zeros((TOKENS, D_MODEL), jnp.float32)
    routed, _ = lax.scan(expert_step, routed_init, (jnp.arange(EXPERTS), w_in, w_out))
    shared_hidden = jax.nn.gelu(jnp.dot(x_tok, shared_in, preferred_element_type=jnp.float32), approximate=True).astype(jnp.bfloat16)
    shared_val = jnp.dot(shared_hidden, shared_out, preferred_element_type=jnp.float32)
    return (routed + shared_val).astype(jnp.bfloat16)
```

```python
import functools

import jax
import jax.numpy as jnp
from jax import lax
from jax.experimental import pallas as pl
from jax.experimental.pallas import tpu as pltpu
from jax.sharding import PartitionSpec as P

LOAD_MULT = 3
MESH = pl.DeviceIdType.MESH
BF = jnp.bfloat16
F32 = jnp.float32
NB1 = 6
NB2 = 8
KH = 256
CB = 256
CH = CB // 2


def gelu(z):
    return 0.5 * z * (1.0 + jnp.tanh(0.7978845608028654 * (z + 0.044715 * (z * z * z))))


def dot(a, b):
    return jnp.dot(a, b, preferred_element_type=F32)


def kernel(top_k, slots, x_hbm, meta_ref, w_in, w_out, sh_in, sh_out, y_ref,
           xall, metaall, hacc, hid, ring1, ring2, xg, disp, comb, obuf, pbuf, r0, r1, r2, s1, s2, acc, zs, shid,
           ag_s, ag_r, mt_s, mt_r, x_sem, g1, g2, p0s, p0r, p1s, p1r, p2s, p2r):
    me = lax.axis_index('ep')
    n_exp, d_model, ff = w_in.shape
    tok = x_hbm.shape[0]
    nh = d_model // KH
    nk = nh // 2
    nb = d_model // CB
    n_sh = sh_in.shape[1] // ff
    core = me % 2
    chip = me // 2
    cx = chip % 2
    cy = chip // 2
    pa = chip * 2 + (1 - core)
    xchip = cy * 2 + (1 - cx)
    ychip = (1 - cy) * 2 + cx
    dchip = (1 - cy) * 2 + (1 - cx)
    xn = xchip * 2 + core
    yn = ychip * 2 + core
    dn = dchip * 2 + core
    n_chunk1 = n_sh * nk + nk * n_exp
    per_b = n_exp + n_sh
    n_chunk2 = nb * per_b
    pre1 = n_sh * nk

    def rcopy(src, dst, ss, rs, dev):
        return pltpu.make_async_remote_copy(src_ref=src, dst_ref=dst, send_sem=ss, recv_sem=rs,
                                            device_id={'ep': dev}, device_id_type=MESH)

    def sh1_copy(i):
        return pltpu.make_async_copy(sh_in.at[pl.ds((i % nk) * 2 * KH, 2 * KH), pl.ds(pl.multiple_of((i // nk) * ff, 128), ff)],
                                     ring1.at[i % NB1], g1.at[i % NB1])

    def ex1_copy(n):
        m = n - pre1
        return pltpu.make_async_copy(w_in.at[m % n_exp, pl.ds((m // n_exp) * 2 * KH, 2 * KH), :], ring1.at[n % NB1], g1.at[n % NB1])

    def next1(n):
        @pl.when(n < pre1)
        def _():
            sh1_copy(n).start()

        @pl.when(jnp.logical_and(n >= pre1, n < n_chunk1))
        def _():
            ex1_copy(n).start()

    def ex2_copy(n):
        return pltpu.make_async_copy(w_out.at[n % per_b, :, pl.ds(pl.multiple_of((n // per_b) * CB, CB), CB)], ring2.at[n % NB2], g2.at[n % NB2])

    def sh2_copy(n):
        return pltpu.make_async_copy(sh_out.at[pl.ds((n % per_b - n_exp) * ff, ff), pl.ds(pl.multiple_of((n // per_b) * CB, CB), CB)],
                                     ring2.at[n % NB2], g2.at[n % NB2])

    def next2(n):
        @pl.when(jnp.logical_and(n < n_chunk2, n % per_b < n_exp))
        def _():
            ex2_copy(n).start()

        @pl.when(jnp.logical_and(n < n_chunk2, n % per_b >= n_exp))
        def _():
            sh2_copy(n).start()

    xin = [pltpu.make_async_copy(x_hbm.at[:, pl.ds(j * KH, KH)], xall.at[j, me], x_sem.at[j]) for j in range(nh)]
    for cp in xin:
        cp.start()
    for i in range(NB1):
        sh1_copy(i).start()

    barrier = pltpu.get_barrier_semaphore()
    for k in range(1, 8):
        pl.semaphore_signal(barrier, inc=1, device_id={'ep': lax.rem(me + k, 8)}, device_id_type=MESH)
    pl.semaphore_wait(barrier, 7)

    def meta_copy(k):
        return rcopy(meta_ref, metaall.at[me], mt_s.at[k - 1], mt_r.at[me], lax.rem(me + k, 8))

    for k in range(1, 8):
        meta_copy(k).start()
    metaall[me] = meta_ref[...]

    sent = []

    def push(j, origin, dev, tag):
        cp = rcopy(xall.at[j, origin], xall.at[j, origin], ag_s.at[j, tag], ag_r.at[j, origin], dev)
        cp.start()
        sent.append(cp)

    def arrived(j, origin):
        rcopy(xall.at[j, origin], xall.at[j, origin], ag_s.at[j, 0], ag_r.at[j, origin], pa).wait_recv()

    def own(j):
        if j < nh:
            push(j, me, xn, 1)
            push(j, me, yn, 2)
            push(j, me, pa, 0)

    def svc(j):
        if j < nh:
            arrived(j, xn)
            if j % 2 == 0:
                push(j, xn, yn, 3)
            push(j, xn, pa, 4)
            arrived(j, yn)
            if j % 2 == 1:
                push(j, yn, xn, 3)
            push(j, yn, pa, 5)
        own(j + 3)
        if j >= 1:
            arrived(j - 1, dn)
            push(j - 1, dn, pa, 6)

    def partner_wait(j):
        for ch in range(4):
            arrived(j, ch * 2 + (1 - core))

    for j in range(nh):
        xin[j].wait()
    for j in range(3):
        own(j)

    zs[...] = jnp.zeros_like(zs)
    def sh_step(i, carry):
        sh1_copy(i).wait()
        kk = i % nk
        lhs = jnp.concatenate([xall[2 * kk, me], xall[2 * kk + 1, me]], axis=1)
        zs[i // nk] += dot(lhs, ring1[i % NB1])
        next1(i + NB1)
        return carry

    lax.fori_loop(0, pre1, sh_step, 0)
    for i in range(n_sh):
        shid[i] = gelu(zs[i]).astype(BF)
    for i in range(NB2):
        next2(jnp.int32(i))

    for k in range(1, 8):
        o = lax.rem(me + k, 8)
        rcopy(meta_ref, metaall.at[o], mt_s.at[k - 1], mt_r.at[o], o).wait_recv()
    t2 = 2 * tok
    upper = (lax.broadcasted_iota(jnp.int32, (t2, t2), 0) < lax.broadcasted_iota(jnp.int32, (t2, t2), 1)).astype(F32).astype(BF)
    expert_id = (lax.broadcasted_iota(jnp.int32, (n_exp, t2), 0) + me * n_exp).astype(F32)
    slot_id = lax.broadcasted_iota(jnp.int32, (slots, t2), 0).astype(F32)
    for q in range(4):
        mq = jnp.concatenate([metaall[2 * q], metaall[2 * q + 1]], axis=1)
        hot = jnp.zeros((n_exp, t2), F32)
        gate = jnp.zeros((n_exp, t2), F32)
        for j in range(top_k):
            eq = mq[j:j + 1, :] == expert_id
            hot += jnp.where(eq, 1.0, 0.0)
            gate += jnp.where(eq, mq[top_k + j:top_k + j + 1, :], 0.0)
        pos = dot(hot.astype(BF), upper)
        code = jnp.where(hot > 0.5, pos, -1.0)
        gated = []
        for e in range(n_exp):
            eq = slot_id == code[e:e + 1, :]
            disp[q, e * slots:(e + 1) * slots, :] = jnp.where(eq, 1.0, 0.0).astype(BF)
            gated.append(jnp.where(eq, gate[e:e + 1, :], 0.0))
        comb[q] = jnp.concatenate(gated, axis=0).T.astype(BF)

    def gather_rows(k):
        for q in range(4):
            for hf in range(2):
                xq = xall[2 * k + hf, 2 * q:2 * q + 2].reshape(t2, KH)
                rows = dot(disp[q], xq).astype(BF)
                for e in range(n_exp):
                    xg[e, q * slots:(q + 1) * slots, hf * KH:(hf + 1) * KH] = rows[e * slots:(e + 1) * slots, :]

    def ex_steps(k, lo, hi):
        def step(e, carry):
            n = pre1 + k * n_exp + e
            ex1_copy(n).wait()
            z = dot(xg[e], ring1[n % NB1])
            if k > 0:
                z += hacc[e]
            if k < nk - 1:
                hacc[e] = z
            else:
                hid[e] = gelu(z).astype(BF)
            next1(n + NB1)
            return carry
        lax.fori_loop(lo, hi, step, 0)

    svc(0)
    svc(1)
    svc(2)
    for k in range(nk):
        partner_wait(2 * k)
        partner_wait(2 * k + 1)
        gather_rows(k)
        ex_steps(k, 0, n_exp // 2)
        if 2 * k + 3 <= nh:
            svc(2 * k + 3)
        ex_steps(k, n_exp // 2, n_exp)
        if 2 * k + 4 <= nh:
            svc(2 * k + 4)

    def c0(b):
        return rcopy(pbuf.at[b % 2, 1 - core], r0.at[b], p0s.at[b], p0r.at[b], pa)

    def c1(b, h):
        return rcopy(s1.at[b, h], r1.at[b, h], p1s.at[b, h], p1r.at[b, h], (xn, yn)[h])

    def c2(b, h):
        return rcopy(s2.at[b, h], r2.at[b, h], p2s.at[b, h], p2r.at[b, h], (yn, xn)[h])

    def svc1(b):
        c0(b).wait_recv()
        slot = b % 2
        lo, hi = slice(0, CH), slice(CH, CB)

        def q_sum(q, cols):
            return pbuf[slot, core, q, :, cols] + r0[b, q, :, cols]

        for i in range(2):
            s1[b, 0, i] = q_sum(i * 2 + (1 - cx), lo)
            s1[b, 1, i] = q_sum((1 - cy) * 2 + i, hi)
        c1(b, 0).start()
        c1(b, 1).start()
        s2[b, 0] = q_sum(ychip, lo)
        s2[b, 1] = q_sum(xchip, hi)
        acc[b, :, lo] += q_sum(chip, lo)
        acc[b, :, hi] += q_sum(chip, hi)
        c0(b).wait_send()

    def svc2(b):
        c1(b, 0).wait_recv()
        s2[b, 0] += r1[b, 0, 1 - cy]
        c2(b, 0).start()
        c1(b, 1).wait_recv()
        s2[b, 1] += r1[b, 1, 1 - cx]
        c2(b, 1).start()
        acc[b, :, :CH] += r1[b, 0, cy]
        acc[b, :, CH:] += r1[b, 1, cx]

    def fin(b):
        c2(b, 0).wait_recv()
        c2(b, 1).wait_recv()
        cols = pl.multiple_of(b * CB, CB)
        y_ref[:, pl.ds(cols, CH)] = (acc[b, :, :CH] + r2[b, 0]).astype(BF)
        y_ref[:, pl.ds(pl.multiple_of(cols + CH, CH), CH)] = (acc[b, :, CH:] + r2[b, 1]).astype(BF)

    def block(b, carry):
        def step(e, c):
            n = b * per_b + e
            ex2_copy(n).wait()
            o = dot(hid[e], ring2[n % NB2]).astype(BF)
            for q in range(4):
                obuf[q, pl.ds(pl.multiple_of(e * slots, 16), slots), :] = o[q * slots:(q + 1) * slots, :]
            next2(n + NB2)
            return c
        lax.fori_loop(0, n_exp, step, 0)
        u = None
        for i in range(n_sh):
            n = b * per_b + n_exp + i
            sh2_copy(n).wait()
            v = dot(shid[i], ring2[n % NB2])
            u = v if u is None else u + v
            next2(n + NB2)
        acc[b] = u
        for q in range(4):
            part = dot(comb[q], obuf[q])
            pbuf[b % 2, 0, q] = part[:tok]
            pbuf[b % 2, 1, q] = part[tok:]
        c0(b).start()

        @pl.when(b >= 1)
        def _():
            svc1(b - 1)

        @pl.when(b >= 2)
        def _():
            svc2(b - 2)

        @pl.when(b >= 4)
        def _():
            fin(b - 4)
        return carry

    lax.fori_loop(0, nb, block, 0)
    svc1(nb - 1)
    svc2(nb - 2)
    fin(nb - 4)
    svc2(nb - 1)
    for b in range(nb - 3, nb):
        fin(b)

    for cp in sent:
        cp.wait_send()
    for k in range(1, 8):
        meta_copy(k).wait_send()
    for b in range(nb):
        for h in range(2):
            c1(b, h).wait_send()
            c2(b, h).wait_send()


def solution(mesh):
    group_size = mesh.shape['ep']

    def local_layer(x_loc, idx_loc, gate_loc, w_in, w_out, shared_in, shared_out):
        tok, top_k = idx_loc.shape
        n_exp, d_model, ff = w_in.shape
        n_sh = shared_in.shape[1] // ff
        cap = min(tok, LOAD_MULT * tok * top_k // (n_exp * group_size))
        slots = -(-2 * cap // 16) * 16
        rows = 4 * slots
        nh, nb = d_model // KH, d_model // CB
        meta = jnp.concatenate([idx_loc.astype(F32).T, gate_loc.T, jnp.zeros((16 - 2 * top_k, tok), F32)], axis=0)
        any_spec = pl.BlockSpec(memory_space=pl.ANY)
        vmem_spec = pl.BlockSpec(memory_space=pltpu.VMEM)
        dma = pltpu.SemaphoreType.DMA
        return pl.pallas_call(
            functools.partial(kernel, top_k, slots),
            out_shape=jax.ShapeDtypeStruct((tok, d_model), BF),
            in_specs=[any_spec, vmem_spec, any_spec, any_spec, any_spec, any_spec],
            out_specs=vmem_spec,
            scratch_shapes=[
                pltpu.VMEM((nh, group_size, tok, KH), BF),
                pltpu.VMEM((group_size, 16, tok), F32),
                pltpu.VMEM((n_exp, rows, ff), F32),
                pltpu.VMEM((n_exp, rows, ff), BF),
                pltpu.VMEM((NB1, 2 * KH, ff), BF),
                pltpu.VMEM((NB2, ff, CB), BF),
                pltpu.VMEM((n_exp, rows, 2 * KH), BF),
                pltpu.VMEM((4, n_exp * slots, 2 * tok), BF),
                pltpu.VMEM((4, 2 * tok, n_exp * slots), BF),
                pltpu.VMEM((4, n_exp * slots, CB), BF),
                pltpu.VMEM((2, 2, 4, tok, CB), F32),
                pltpu.VMEM((nb, 4, tok, CB), F32),
                pltpu.VMEM((nb, 2, 2, tok, CH), F32),
                pltpu.VMEM((nb, 2, tok, CH), F32),
                pltpu.VMEM((nb, 2, 2, tok, CH), F32),
                pltpu.VMEM((nb, 2, tok, CH), F32),
                pltpu.VMEM((nb, tok, CB), F32),
                pltpu.VMEM((n_sh, tok, ff), F32),
                pltpu.VMEM((n_sh, tok, ff), BF),
                dma((nh, 7)), dma((nh, 8)), dma((7,)), dma((8,)), dma((nh,)), dma((NB1,)), dma((NB2,)),
                dma((nb,)), dma((nb,)), dma((nb, 2)), dma((nb, 2)), dma((nb, 2)), dma((nb, 2)),
            ],
            compiler_params=pltpu.CompilerParams(collective_id=0, has_side_effects=True, vmem_limit_bytes=67043328),
        )(x_loc, meta, w_in, w_out, shared_in, shared_out)

    tok_spec = P(('dp', 'ep'), None)
    expert_spec = P('ep', None, None)
    whole_spec = P(None, None)
    return jax.shard_map(local_layer, mesh=mesh, in_specs=(tok_spec, tok_spec, tok_spec, expert_spec, expert_spec, whole_spec, whole_spec), out_specs=tok_spec, check_vma=False)
```

```python
import functools

import jax
import jax.numpy as jnp
from jax import lax
from jax.experimental import pallas as pl
from jax.experimental.pallas import tpu as pltpu
from jax.sharding import PartitionSpec as P

LOAD_MULT = 3
MESH = pl.DeviceIdType.MESH
BF = jnp.bfloat16
F32 = jnp.float32
NB1 = 8
GRP = 2
KH = 256
CB = 256
CH = CB // 2


def gelu(z):
    half = 0.5 * z
    return half + half * jnp.tanh(z * (0.7978845608028654 + 0.03567740813636141 * (z * z)))


def dot(a, b):
    return jnp.dot(a, b, preferred_element_type=F32)


def kernel(top_k, slots, x_hbm, idx_ref, gate_ref, w_in, w_out, sh_in, sh_out, y_ref,
           xall, idxall, gateall, hacc, hid, ring1, ring2, xg, disp, comb, obuf, pbuf, r0, r1, r2, s1, s2, acc, shid,
           ag_s, ag_r, mi_s, mi_r, mg_s, mg_r, x_sem, g1, g2, p0s, p0r, p1s, p1r, p2s, p2r):
    me = lax.axis_index('ep')
    n_exp, d_model, ff = w_in.shape
    tok = x_hbm.shape[0]
    nh = d_model // KH
    nk = nh // 2
    nb = d_model // CB
    n_sh = sh_in.shape[1] // ff
    per = n_exp // n_sh
    core = me % 2
    chip = me // 2
    cx = chip % 2
    cy = chip // 2
    pa = chip * 2 + (1 - core)
    xchip = cy * 2 + (1 - cx)
    ychip = (1 - cy) * 2 + cx
    dchip = (1 - cy) * 2 + (1 - cx)
    xn = xchip * 2 + core
    yn = ychip * 2 + core
    dn = dchip * 2 + core
    pre1 = n_sh * nk
    n_chunk1 = pre1 + nk * n_exp

    def rcopy(src, dst, ss, rs, dev):
        return pltpu.make_async_remote_copy(src_ref=src, dst_ref=dst, send_sem=ss, recv_sem=rs,
                                            device_id={'ep': dev}, device_id_type=MESH)

    def copy1(n):
        slot = n % NB1
        if n < pre1:
            src = sh_in.at[pl.ds((n % nk) * 2 * KH, 2 * KH), pl.ds((n // nk) * ff, ff)]
        else:
            m = n - pre1
            src = w_in.at[m % n_exp, pl.ds((m // n_exp) * 2 * KH, 2 * KH), :]
        return pltpu.make_async_copy(src, ring1.at[slot], g1.at[slot])

    def start1(n):
        if n < n_chunk1:
            copy1(n).start()

    def copy2s(half, i):
        src = sh_out.at[pl.ds((i // per) * ff, ff), pl.ds((half * per + i % per) * CB, CB)]
        return pltpu.make_async_copy(src, ring2.at[half, i], g2.at[half, i])

    def copy2(b, e):
        src = w_out.at[e, :, pl.ds(pl.multiple_of(b * CB, CB), CB)]
        return pltpu.make_async_copy(src, ring2.at[b % 2, e], g2.at[b % 2, e])

    xin = [pltpu.make_async_copy(x_hbm.at[:, pl.ds(j * KH, KH)], xall.at[j, me], x_sem.at[j]) for j in range(nh)]
    for cp in xin:
        cp.start()
    for i in range(NB1):
        start1(i)

    barrier = pltpu.get_barrier_semaphore()
    for k in range(1, 8):
        pl.semaphore_signal(barrier, inc=1, device_id={'ep': lax.rem(me + k, 8)}, device_id_type=MESH)
    for half in range(2):
        for i in range(n_exp):
            copy2s(half, i).start()
    for cp in xin:
        cp.wait()
    pl.semaphore_wait(barrier, 7)

    sent = []

    def push(j, origin, dev, tag):
        cp = rcopy(xall.at[j, origin], xall.at[j, origin], ag_s.at[j, tag], ag_r.at[j, origin], dev)
        cp.start()
        sent.append(cp)

    def arrived(j, origin):
        rcopy(xall.at[j, origin], xall.at[j, origin], ag_s.at[j, 0], ag_r.at[j, origin], pa).wait_recv()

    def own(j):
        push(j, me, xn, 1)
        push(j, me, yn, 2)
        push(j, me, dn, 3)
        push(j, me, pa, 0)

    def svc_a(j):
        if j < nh:
            arrived(j, xn)
            push(j, xn, pa, 4)
            arrived(j, yn)
            push(j, yn, pa, 5)

    def svc_d(j):
        if j < nh:
            arrived(j, dn)
            push(j, dn, pa, 6)

    def partner_wait(j):
        for ch in range(4):
            arrived(j, ch * 2 + (1 - core))

    own(0)

    def meta_copies(k, o):
        dev = lax.rem(me + k, 8)
        return (rcopy(idx_ref, idxall.at[o], mi_s.at[k - 1], mi_r.at[o], dev),
                rcopy(gate_ref, gateall.at[o], mg_s.at[k - 1], mg_r.at[o], dev))

    for k in range(1, 8):
        for cp in meta_copies(k, me):
            cp.start()
    idxall[me] = idx_ref[...]
    gateall[me] = gate_ref[...]
    for j in range(1, nh):
        own(j)

    xk = [jnp.concatenate([xall[2 * k, me], xall[2 * k + 1, me]], axis=1) for k in range(nk)]
    for i in range(n_sh):
        z = None
        for k in range(nk):
            copy1(i * nk + k).wait()
        for k in range(nk):
            v = dot(xk[k], ring1[(i * nk + k) % NB1])
            z = v if z is None else z + v
        shid[i] = gelu(z).astype(BF)
        for k in range(nk):
            start1(i * nk + k + NB1)

    def sh_out_half(half):
        for i in range(n_exp):
            copy2s(half, i).wait()
        for i in range(per):
            acc[half * per + i] = sum(dot(shid[m], ring2[half, m * per + i]) for m in range(n_sh))
        for e in range(n_exp):
            copy2(half, e).start()

    svc_a(0)
    svc_d(0)

    for k in range(1, 8):
        for cp in meta_copies(k, lax.rem(me + k, 8)):
            cp.wait_recv()
    t2 = 2 * tok
    upper = (lax.broadcasted_iota(jnp.int32, (t2, t2), 0) < lax.broadcasted_iota(jnp.int32, (t2, t2), 1)).astype(F32).astype(BF)
    expert_id = lax.broadcasted_iota(jnp.int32, (n_exp, t2), 0) + me * n_exp
    slot_id = lax.broadcasted_iota(jnp.int32, (slots, t2), 0).astype(F32)
    for q in range(4):
        iq = jnp.concatenate([idxall[2 * q], idxall[2 * q + 1]], axis=1)
        gq = jnp.concatenate([gateall[2 * q], gateall[2 * q + 1]], axis=1)
        hot = jnp.zeros((n_exp, t2), F32)
        gate = jnp.zeros((n_exp, t2), F32)
        for j in range(top_k):
            eq = iq[j:j + 1, :] == expert_id
            hot += jnp.where(eq, 1.0, 0.0)
            gate += jnp.where(eq, gq[j:j + 1, :], 0.0)
        pos = dot(hot.astype(BF), upper)
        code = jnp.where(hot > 0.5, pos, -1.0)
        gated = []
        for e in range(n_exp):
            eq = slot_id == code[e:e + 1, :]
            disp[q, e * slots:(e + 1) * slots, :] = jnp.where(eq, 1.0, 0.0).astype(BF)
            gated.append(jnp.where(eq, gate[e:e + 1, :], 0.0))
        comb[q] = jnp.concatenate(gated, axis=0).T.astype(BF)

    svc_a(1)
    svc_d(1)

    def gather_rows(k):
        for q in range(4):
            for hf in range(2):
                xq = xall[2 * k + hf, 2 * q:2 * q + 2].reshape(t2, KH)
                rows = dot(disp[q], xq).astype(BF)
                for e in range(n_exp):
                    xg[e, q * slots:(q + 1) * slots, hf * KH:(hf + 1) * KH] = rows[e * slots:(e + 1) * slots, :]

    def ex_groups(k, lo, hi):
        def group(g, carry):
            base = pre1 + k * n_exp + g * GRP

            def copy(i):
                n = base + i
                m = n - pre1
                src = w_in.at[m % n_exp, pl.ds((m // n_exp) * 2 * KH, 2 * KH), :]
                return pltpu.make_async_copy(src, ring1.at[n % NB1], g1.at[n % NB1])

            for i in range(GRP):
                copy(i).wait()
            for i in range(GRP):
                e = g * GRP + i
                z = dot(xg[e], ring1[(base + i) % NB1])
                if k > 0:
                    z += hacc[e]
                if k < nk - 1:
                    hacc[e] = z
                else:
                    hid[e] = gelu(z).astype(BF)

            @pl.when(base + NB1 < n_chunk1)
            def _():
                for i in range(GRP):
                    copy(i + NB1).start()
            return carry
        lax.fori_loop(lo, hi, group, 0)

    sh_out_half(0)
    sh_out_half(1)
    half_g = n_exp // GRP // 2
    svc_a(2)
    svc_d(2)
    for k in range(nk):
        partner_wait(2 * k)
        partner_wait(2 * k + 1)
        gather_rows(k)
        ex_groups(k, 0, half_g)
        svc_a(2 * k + 3)
        svc_d(2 * k + 3)
        ex_groups(k, half_g, 2 * half_g)
        svc_a(2 * k + 4)
        svc_d(2 * k + 4)

    def c0(b):
        return rcopy(pbuf.at[b % 2, 1 - core], r0.at[b % 4], p0s.at[b], p0r.at[b], pa)

    def c1(b, h):
        return rcopy(s1.at[b % 4, h], r1.at[b % 4, h], p1s.at[b, h], p1r.at[b, h], (xn, yn)[h])

    def c2(b, h):
        return rcopy(s2.at[b % 4, h], r2.at[b % 4, h], p2s.at[b, h], p2r.at[b, h], (yn, xn)[h])

    def svc1(b):
        c0(b).wait_recv()
        slot = b % 2
        rs = b % 4
        lo, hi = slice(0, CH), slice(CH, CB)

        def q_sum(q, cols):
            return pbuf[slot, core, q, :, cols] + r0[rs, q, :, cols]

        for i in range(2):
            s1[rs, 0, i] = q_sum(i * 2 + (1 - cx), lo)
            s1[rs, 1, i] = q_sum((1 - cy) * 2 + i, hi)
        c1(b, 0).start()
        c1(b, 1).start()
        s2[rs, 0] = q_sum(ychip, lo)
        s2[rs, 1] = q_sum(xchip, hi)
        acc[b, :, lo] += q_sum(chip, lo)
        acc[b, :, hi] += q_sum(chip, hi)
        c0(b).wait_send()

    def svc2(b):
        rs = b % 4
        c1(b, 0).wait_recv()
        c1(b, 1).wait_recv()
        s2[rs, 0] += r1[rs, 0, 1 - cy]
        c2(b, 0).start()
        s2[rs, 1] += r1[rs, 1, 1 - cx]
        c2(b, 1).start()
        acc[b, :, :CH] += r1[rs, 0, cy]
        acc[b, :, CH:] += r1[rs, 1, cx]

    def sends_done(b):
        for h in range(2):
            c1(b, h).wait_send()
            c2(b, h).wait_send()

    def fin(b):
        c2(b, 0).wait_recv()
        c2(b, 1).wait_recv()
        cols = pl.multiple_of(b * CB, CB)
        y_ref[:, pl.ds(cols, CH)] = (acc[b, :, :CH] + r2[b % 4, 0]).astype(BF)
        y_ref[:, pl.ds(pl.multiple_of(cols + CH, CH), CH)] = (acc[b, :, CH:] + r2[b % 4, 1]).astype(BF)

    def block(b, carry):
        for e in range(n_exp):
            copy2(b, e).wait()
        for e in range(n_exp):
            o = dot(hid[e], ring2[b % 2, e]).astype(BF)
            for q in range(4):
                obuf[q, e * slots:(e + 1) * slots, :] = o[q * slots:(q + 1) * slots, :]
        for q in range(4):
            part = dot(comb[q], obuf[q])
            pbuf[b % 2, 0, q] = part[:tok]
            pbuf[b % 2, 1, q] = part[tok:]
        c0(b).start()

        @pl.when(b + 2 < nb)
        def _():
            for e in range(n_exp):
                copy2(b + 2, e).start()

        @pl.when(b >= 5)
        def _():
            sends_done(b - 5)

        @pl.when(b >= 1)
        def _():
            svc1(b - 1)

        @pl.when(b >= 2)
        def _():
            svc2(b - 2)

        @pl.when(b >= 4)
        def _():
            fin(b - 4)
        return carry

    lax.fori_loop(0, nb, block, 0)
    sends_done(nb - 5)
    svc1(nb - 1)
    svc2(nb - 2)
    fin(nb - 4)
    svc2(nb - 1)
    for b in range(nb - 3, nb):
        fin(b)

    for cp in sent:
        cp.wait_send()
    for k in range(1, 8):
        for cp in meta_copies(k, me):
            cp.wait_send()
    for b in range(nb - 4, nb):
        sends_done(b)


def solution(mesh):
    group_size = mesh.shape['ep']

    def local_layer(x_loc, idx_loc, gate_loc, w_in, w_out, shared_in, shared_out):
        tok, top_k = idx_loc.shape
        n_exp, d_model, ff = w_in.shape
        n_sh = shared_in.shape[1] // ff
        cap = min(tok, LOAD_MULT * tok * top_k // (n_exp * group_size))
        slots = -(-2 * cap // 16) * 16
        rows = 4 * slots
        nh, nb = d_model // KH, d_model // CB
        any_spec = pl.BlockSpec(memory_space=pl.ANY)
        vmem_spec = pl.BlockSpec(memory_space=pltpu.VMEM)
        dma = pltpu.SemaphoreType.DMA
        return pl.pallas_call(
            functools.partial(kernel, top_k, slots),
            out_shape=jax.ShapeDtypeStruct((tok, d_model), BF),
            in_specs=[any_spec, vmem_spec, vmem_spec, any_spec, any_spec, any_spec, any_spec],
            out_specs=vmem_spec,
            scratch_shapes=[
                pltpu.VMEM((nh, group_size, tok, KH), BF),
                pltpu.VMEM((group_size, top_k, tok), jnp.int32),
                pltpu.VMEM((group_size, top_k, tok), F32),
                pltpu.VMEM((n_exp, rows, ff), F32),
                pltpu.VMEM((n_exp, rows, ff), BF),
                pltpu.VMEM((NB1, 2 * KH, ff), BF),
                pltpu.VMEM((2, n_exp, ff, CB), BF),
                pltpu.VMEM((n_exp, rows, 2 * KH), BF),
                pltpu.VMEM((4, n_exp * slots, 2 * tok), BF),
                pltpu.VMEM((4, 2 * tok, n_exp * slots), BF),
                pltpu.VMEM((4, n_exp * slots, CB), BF),
                pltpu.VMEM((2, 2, 4, tok, CB), F32),
                pltpu.VMEM((4, 4, tok, CB), F32),
                pltpu.VMEM((4, 2, 2, tok, CH), F32),
                pltpu.VMEM((4, 2, tok, CH), F32),
                pltpu.VMEM((4, 2, 2, tok, CH), F32),
                pltpu.VMEM((4, 2, tok, CH), F32),
                pltpu.VMEM((nb, tok, CB), F32),
                pltpu.VMEM((n_sh, tok, ff), BF),
                dma((nh, 7)), dma((nh, 8)), dma((7,)), dma((8,)), dma((7,)), dma((8,)), dma((nh,)), dma((NB1,)), dma((2, n_exp)),
                dma((nb,)), dma((nb,)), dma((nb, 2)), dma((nb, 2)), dma((nb, 2)), dma((nb, 2)),
            ],
            compiler_params=pltpu.CompilerParams(collective_id=0, has_side_effects=True, vmem_limit_bytes=67043328),
        )(x_loc, idx_loc.T, gate_loc.T, w_in, w_out, shared_in, shared_out)

    tok_spec = P(('dp', 'ep'), None)
    expert_spec = P('ep', None, None)
    whole_spec = P(None, None)
    return jax.shard_map(local_layer, mesh=mesh, in_specs=(tok_spec, tok_spec, tok_spec, expert_spec, expert_spec, whole_spec, whole_spec), out_specs=tok_spec, check_vma=False)
```

```python
import functools

import jax
import jax.numpy as jnp
from jax import lax
from jax.experimental import pallas as pl
from jax.experimental.pallas import tpu as pltpu
from jax.sharding import PartitionSpec as P

LOAD_MULT = 3
MESH = pl.DeviceIdType.MESH
BF = jnp.bfloat16
F32 = jnp.float32
NB1 = 8
MID = 6
NB = 768
GRP = 2
KH = 256
CB = 256
CH = CB // 2


def gelu(z):
    half = 0.5 * z
    return half + half * jnp.tanh(z * (0.7978845608028654 + 0.03567740813636141 * (z * z)))


def dot(a, b):
    return jnp.dot(a, b, preferred_element_type=F32)


def kernel(top_k, slots, x_hbm, idx_hbm, gate_hbm, w_in, w_out, sh_in, sh_out, y_hbm,
           xall, idxall, gateall, hacc, hid, ring1, ring2, xg, disp, comb, obuf, pbuf, r0, r1, r2, s1, s2, acc, shid, ybuf,
           ag_s, ag_r, mi_s, mi_r, mg_s, mg_r, m_sem, y_sem, x_sem, g1, g2, p0s, p0r, p1s, p1r, p2s, p2r):
    me = lax.axis_index('ep')
    n_exp, d_model, ff = w_in.shape
    tok = x_hbm.shape[0]
    nh = d_model // KH
    nk = nh // 2
    nb = d_model // CB
    n_sh = sh_in.shape[1] // ff
    per = n_exp // n_sh
    core = me % 2
    chip = me // 2
    cx = chip % 2
    cy = chip // 2
    pa = chip * 2 + (1 - core)
    xchip = cy * 2 + (1 - cx)
    ychip = (1 - cy) * 2 + cx
    dchip = (1 - cy) * 2 + (1 - cx)
    xn = xchip * 2 + core
    yn = ychip * 2 + core
    dn = dchip * 2 + core
    pre1 = n_sh * nk
    n_chunk1 = pre1 + nk * n_exp

    def rcopy(src, dst, ss, rs, dev):
        return pltpu.make_async_remote_copy(src_ref=src, dst_ref=dst, send_sem=ss, recv_sem=rs,
                                            device_id={'ep': dev}, device_id_type=MESH)

    def copy1(n):
        slot = n % NB1
        if n < pre1:
            src = sh_in.at[pl.ds((n % nk) * 2 * KH, 2 * KH), pl.ds((n // nk) * ff, ff)]
        else:
            m = n - pre1
            src = w_in.at[m % n_exp, pl.ds((m // n_exp) * 2 * KH, 2 * KH), :]
        return pltpu.make_async_copy(src, ring1.at[slot], g1.at[slot])

    def start1(n):
        if n < n_chunk1:
            copy1(n).start()

    def copy2s(half, i):
        src = sh_out.at[pl.ds((i // per) * ff, ff), pl.ds((half * per + i % per) * CB, CB)]
        return pltpu.make_async_copy(src, ring2.at[half, i], g2.at[half, i])

    def copy2(b, e):
        src = w_out.at[e, :, pl.ds(pl.multiple_of(b * CB, CB), CB)]
        return pltpu.make_async_copy(src, ring2.at[b % 2, e], g2.at[b % 2, e])

    xin = [pltpu.make_async_copy(x_hbm.at[:, pl.ds(j * KH, KH)], xall.at[j, me], x_sem.at[j]) for j in range(nh)]
    routing = (pltpu.make_async_copy(idx_hbm, idxall.at[me], m_sem.at[0]),
               pltpu.make_async_copy(gate_hbm, gateall.at[me], m_sem.at[1]))
    for cp in routing:
        cp.start()
    for cp in xin:
        cp.start()
    for i in range(NB1):
        start1(i)

    barrier = pltpu.get_barrier_semaphore()
    for k in range(1, 8):
        pl.semaphore_signal(barrier, inc=1, device_id={'ep': lax.rem(me + k, 8)}, device_id_type=MESH)
    for half in range(2):
        for i in range(n_exp):
            copy2s(half, i).start()
    for cp in xin:
        cp.wait()
    for cp in routing:
        cp.wait()
    pl.semaphore_wait(barrier, 7)

    sent = []

    def push(j, origin, dev, tag):
        cp = rcopy(xall.at[j, origin], xall.at[j, origin], ag_s.at[j, tag], ag_r.at[j, origin], dev)
        cp.start()
        sent.append(cp)

    def arrived(j, origin):
        rcopy(xall.at[j, origin], xall.at[j, origin], ag_s.at[j, 0], ag_r.at[j, origin], pa).wait_recv()

    def own(j):
        push(j, me, xn, 1)
        push(j, me, yn, 2)
        push(j, me, dn, 3)
        push(j, me, pa, 0)

    def svc_a(j):
        if j < nh:
            arrived(j, xn)
            push(j, xn, pa, 4)
            arrived(j, yn)
            push(j, yn, pa, 5)

    def svc_d(j):
        if j < nh:
            arrived(j, dn)
            push(j, dn, pa, 6)

    def partner_wait(j):
        for ch in range(4):
            arrived(j, ch * 2 + (1 - core))

    own(0)

    def meta_copies(k, o):
        dev = lax.rem(me + k, 8)
        return (rcopy(idxall.at[o], idxall.at[o], mi_s.at[k - 1], mi_r.at[o], dev),
                rcopy(gateall.at[o], gateall.at[o], mg_s.at[k - 1], mg_r.at[o], dev))

    for k in range(1, 8):
        for cp in meta_copies(k, me):
            cp.start()
    for j in range(1, nh):
        own(j)

    xk = [jnp.concatenate([xall[2 * k, me], xall[2 * k + 1, me]], axis=1) for k in range(nk)]
    for i in range(n_sh):
        z = None
        for k in range(nk):
            copy1(i * nk + k).wait()
        for k in range(nk):
            v = dot(xk[k], ring1[(i * nk + k) % NB1])
            z = v if z is None else z + v
        shid[i] = gelu(z).astype(BF)
        for k in range(nk):
            start1(i * nk + k + NB1)

    def sh_out_half(half):
        for i in range(n_exp):
            copy2s(half, i).wait()
        for i in range(per):
            acc[half * per + i] = sum(dot(shid[m], ring2[half, m * per + i]) for m in range(n_sh))
        for e in range(n_exp):
            copy2(half, e).start()

    svc_a(0)
    svc_d(0)

    for k in range(1, 8):
        for cp in meta_copies(k, lax.rem(me + k, 8)):
            cp.wait_recv()
    t2 = 2 * tok
    upper = (lax.broadcasted_iota(jnp.int32, (t2, t2), 0) < lax.broadcasted_iota(jnp.int32, (t2, t2), 1)).astype(F32).astype(BF)
    expert_id = lax.broadcasted_iota(jnp.int32, (n_exp, t2), 0) + me * n_exp
    slot_id = lax.broadcasted_iota(jnp.int32, (slots, t2), 0).astype(F32)
    for q in range(4):
        iq = jnp.concatenate([idxall[2 * q], idxall[2 * q + 1]], axis=1)
        gq = jnp.concatenate([gateall[2 * q], gateall[2 * q + 1]], axis=1)
        hot = jnp.zeros((n_exp, t2), F32)
        gate = jnp.zeros((n_exp, t2), F32)
        for j in range(top_k):
            eq = iq[j:j + 1, :] == expert_id
            hot += jnp.where(eq, 1.0, 0.0)
            gate += jnp.where(eq, gq[j:j + 1, :], 0.0)
        pos = dot(hot.astype(BF), upper)
        code = jnp.where(hot > 0.5, pos, -1.0)
        gated = []
        for e in range(n_exp):
            eq = slot_id == code[e:e + 1, :]
            disp[q, e * slots:(e + 1) * slots, :] = jnp.where(eq, 1.0, 0.0).astype(BF)
            gated.append(jnp.where(eq, gate[e:e + 1, :], 0.0))
        comb[q] = jnp.concatenate(gated, axis=0).T.astype(BF)

    svc_a(1)
    svc_d(1)

    def gather_rows(k):
        for q in range(4):
            for hf in range(2):
                xq = xall[2 * k + hf, 2 * q:2 * q + 2].reshape(t2, KH)
                rows = dot(disp[q], xq).astype(BF)
                for e in range(n_exp):
                    xg[e, q * slots:(q + 1) * slots, hf * KH:(hf + 1) * KH] = rows[e * slots:(e + 1) * slots, :]

    def ex_groups(k, lo, hi):
        def group(g, carry):
            base = pre1 + k * n_exp + g * GRP

            def copy(i):
                n = base + i
                m = n - pre1
                src = w_in.at[m % n_exp, pl.ds((m // n_exp) * 2 * KH, 2 * KH), :]
                return pltpu.make_async_copy(src, ring1.at[n % NB1], g1.at[n % NB1])

            for i in range(GRP):
                copy(i).wait()
            for i in range(GRP):
                e = g * GRP + i
                for col in range(0, ff, NB):
                    ns = slice(col, min(col + NB, ff))
                    z = dot(xg[e], ring1[(base + i) % NB1, :, ns])
                    if k > 0:
                        z += hacc[e, :, ns]
                    if k < nk - 1:
                        hacc[e, :, ns] = z
                    else:
                        hid[e, :, ns] = gelu(z).astype(BF)

            @pl.when(base + NB1 < n_chunk1)
            def _():
                for i in range(GRP):
                    copy(i + NB1).start()
            return carry
        lax.fori_loop(lo, hi, group, 0)

    sh_out_half(0)
    sh_out_half(1)
    half_g = n_exp // GRP // 2
    for k in range(nk):
        partner_wait(2 * k)
        partner_wait(2 * k + 1)
        gather_rows(k)
        if k == 0:
            svc_a(2)
            svc_d(2)
        ex_groups(k, 0, half_g)
        svc_a(2 * k + 3)
        svc_d(2 * k + 3)
        ex_groups(k, half_g, 2 * half_g)
        svc_a(2 * k + 4)
        svc_d(2 * k + 4)

    def c0(b):
        return rcopy(pbuf.at[b % 2, 1 - core], r0.at[b % 4], p0s.at[b], p0r.at[b], pa)

    def c1(b, h):
        return rcopy(s1.at[b % 4, h], r1.at[b % 4, h], p1s.at[b, h], p1r.at[b, h], (xn, yn)[h])

    def c2(b, h):
        return rcopy(s2.at[b % 4, h], r2.at[b % 4, h], p2s.at[b, h], p2r.at[b, h], (yn, xn)[h])

    def svc1(b):
        c0(b).wait_recv()
        slot = b % 2
        rs = b % 4
        lo, hi = slice(0, CH), slice(CH, CB)

        def q_sum(q, cols):
            return pbuf[slot, core, q, :, cols] + r0[rs, q, :, cols]

        for i in range(2):
            s1[rs, 0, i] = q_sum(i * 2 + (1 - cx), lo)
            s1[rs, 1, i] = q_sum((1 - cy) * 2 + i, hi)
        c1(b, 0).start()
        c1(b, 1).start()
        s2[rs, 0] = q_sum(ychip, lo)
        s2[rs, 1] = q_sum(xchip, hi)
        acc[b, :, lo] += q_sum(chip, lo)
        acc[b, :, hi] += q_sum(chip, hi)
        c0(b).wait_send()

    def svc2(b):
        rs = b % 4
        c1(b, 0).wait_recv()
        c1(b, 1).wait_recv()
        s2[rs, 0] += r1[rs, 0, 1 - cy]
        c2(b, 0).start()
        s2[rs, 1] += r1[rs, 1, 1 - cx]
        c2(b, 1).start()
        acc[b, :, :CH] += r1[rs, 0, cy]
        acc[b, :, CH:] += r1[rs, 1, cx]

    def sends_done(b):
        for h in range(2):
            c1(b, h).wait_send()
            c2(b, h).wait_send()

    def out_copy(b):
        return pltpu.make_async_copy(ybuf.at[b], y_hbm.at[:, pl.ds(pl.multiple_of(b * CB, CB), CB)], y_sem.at[b])

    def fin(b):
        c2(b, 0).wait_recv()
        c2(b, 1).wait_recv()
        ybuf[b, :, :CH] = (acc[b, :, :CH] + r2[b % 4, 0]).astype(BF)
        ybuf[b, :, CH:] = (acc[b, :, CH:] + r2[b % 4, 1]).astype(BF)
        out_copy(b).start()

    def block(b, carry):
        for e in range(n_exp):
            copy2(b, e).wait()
        for e in range(n_exp):
            if e == MID:
                @pl.when(b >= 5)
                def _():
                    sends_done(b - 5)

                @pl.when(b >= 1)
                def _():
                    svc1(b - 1)

            o = dot(hid[e], ring2[b % 2, e]).astype(BF)
            for q in range(4):
                obuf[q, e * slots:(e + 1) * slots, :] = o[q * slots:(q + 1) * slots, :]
        for q in range(4):
            part = dot(comb[q], obuf[q])
            pbuf[b % 2, 0, q] = part[:tok]
            pbuf[b % 2, 1, q] = part[tok:]
        c0(b).start()

        @pl.when(b + 2 < nb)
        def _():
            for e in range(n_exp):
                copy2(b + 2, e).start()

        @pl.when(b >= 2)
        def _():
            svc2(b - 2)

        @pl.when(b >= 4)
        def _():
            fin(b - 4)
        return carry

    lax.fori_loop(0, nb, block, 0)
    sends_done(nb - 5)
    svc1(nb - 1)
    svc2(nb - 2)
    fin(nb - 4)
    svc2(nb - 1)
    for b in range(nb - 3, nb):
        fin(b)

    for cp in sent:
        cp.wait_send()
    for k in range(1, 8):
        for cp in meta_copies(k, me):
            cp.wait_send()
    for b in range(nb - 4, nb):
        sends_done(b)
    for b in range(nb):
        out_copy(b).wait()


def solution(mesh):
    group_size = mesh.shape['ep']

    def local_layer(x_loc, idx_loc, gate_loc, w_in, w_out, shared_in, shared_out):
        tok, top_k = idx_loc.shape
        n_exp, d_model, ff = w_in.shape
        n_sh = shared_in.shape[1] // ff
        cap = min(tok, LOAD_MULT * tok * top_k // (n_exp * group_size))
        slots = -(-2 * cap // 16) * 16
        rows = 4 * slots
        nh, nb = d_model // KH, d_model // CB
        any_spec = pl.BlockSpec(memory_space=pl.ANY)
        dma = pltpu.SemaphoreType.DMA
        return pl.pallas_call(
            functools.partial(kernel, top_k, slots),
            out_shape=jax.ShapeDtypeStruct((tok, d_model), BF),
            in_specs=[any_spec, any_spec, any_spec, any_spec, any_spec, any_spec, any_spec],
            out_specs=any_spec,
            scratch_shapes=[
                pltpu.VMEM((nh, group_size, tok, KH), BF),
                pltpu.VMEM((group_size, top_k, tok), jnp.int32),
                pltpu.VMEM((group_size, top_k, tok), F32),
                pltpu.VMEM((n_exp, rows, ff), F32),
                pltpu.VMEM((n_exp, rows, ff), BF),
                pltpu.VMEM((NB1, 2 * KH, ff), BF),
                pltpu.VMEM((2, n_exp, ff, CB), BF),
                pltpu.VMEM((n_exp, rows, 2 * KH), BF),
                pltpu.VMEM((4, n_exp * slots, 2 * tok), BF),
                pltpu.VMEM((4, 2 * tok, n_exp * slots), BF),
                pltpu.VMEM((4, n_exp * slots, CB), BF),
                pltpu.VMEM((2, 2, 4, tok, CB), F32),
                pltpu.VMEM((4, 4, tok, CB), F32),
                pltpu.VMEM((4, 2, 2, tok, CH), F32),
                pltpu.VMEM((4, 2, tok, CH), F32),
                pltpu.VMEM((4, 2, 2, tok, CH), F32),
                pltpu.VMEM((4, 2, tok, CH), F32),
                pltpu.VMEM((nb, tok, CB), F32),
                pltpu.VMEM((n_sh, tok, ff), BF),
                pltpu.VMEM((nb, tok, CB), BF),
                dma((nh, 7)), dma((nh, 8)), dma((7,)), dma((8,)), dma((7,)), dma((8,)), dma((2,)), dma((nb,)), dma((nh,)), dma((NB1,)), dma((2, n_exp)),
                dma((nb,)), dma((nb,)), dma((nb, 2)), dma((nb, 2)), dma((nb, 2)), dma((nb, 2)),
            ],
            compiler_params=pltpu.CompilerParams(collective_id=0, has_side_effects=True, vmem_limit_bytes=67043328),
        )(x_loc, idx_loc.T, gate_loc.T, w_in, w_out, shared_in, shared_out)

    tok_spec = P(('dp', 'ep'), None)
    expert_spec = P('ep', None, None)
    whole_spec = P(None, None)
    return jax.shard_map(local_layer, mesh=mesh, in_specs=(tok_spec, tok_spec, tok_spec, expert_spec, expert_spec, whole_spec, whole_spec), out_specs=tok_spec, check_vma=False)
```
